64 devices in a mesh: dp: 8 (over x, y, core), tp: 8 (over z).
Axes of the slice: x: 2, y: 2, z: 8, core: 2. Of those that a mesh axis runs over, the one named last changes fastest.
The devices are a block of a 4x4x8 slice.
Arguments:
- x: bfloat16 [14336, 5120], P(('dp', 'tp')), parts along dimension 0
- w_gate: bfloat16 [5120, 17408], P(None, 'tp')
- w_up: bfloat16 [5120, 17408], P(None, 'tp')
- w_down: bfloat16 [17408, 5120], P('tp')
Outputs:
- output: bfloat16 [14336, 5120], P(('dp', 'tp')), parts along dimension 0
There are 8 independent parts. The reference program is written for one: setup_inputs(seed, part) draws one part's arguments, and reference() takes and returns one part's arrays. A program takes and returns all parts, laid end to end along the dimension named above; an argument that names none is the same for every part.
All inputs are finite; a program needn't handle non-finite values.
Results may differ from the reference program's by a relative error of at most 0.016.
Values are sent between devices in bfloat16 or wider.
A program may use at most 768 MiB of HBM per device.

```python
import jax
import jax.numpy as jnp

ROWS = 1792
D = 5120
FF = 17408


def setup_inputs(seed: int = 0, part: int = 0) -> dict:
    kx, kg, ku, kd = jax.random.split(jax.random.key(seed), 4)
    drawn = {
        "x": jax.random.normal(jax.random.fold_in(kx, part), (ROWS, D), jnp.float32),
        "w_gate": jax.random.normal(kg, (D, FF), jnp.float32) * D**-0.5,
        "w_up": jax.random.normal(ku, (D, FF), jnp.float32) * D**-0.5,
        "w_down": jax.random.normal(kd, (FF, D), jnp.float32) * FF**-0.5,
    }
    return {k: v.astype(jnp.bfloat16) for k, v in drawn.items()}


def reference(x, w_gate, w_up, w_down):
    gate = jnp.dot(x, w_gate, preferred_element_type=jnp.float32)
    up = jnp.dot(x, w_up, preferred_element_type=jnp.float32)
    hidden = (jax.nn.silu(gate) * up).astype(jnp.bfloat16)
    return jnp.dot(hidden, w_down, preferred_element_type=jnp.float32).astype(jnp.bfloat16)
```

```python
import functools

import jax
import jax.numpy as jnp
from jax import lax
from jax.experimental import pallas as pl
from jax.experimental.pallas import tpu as pltpu
from jax.sharding import PartitionSpec as P

LANES = 128
PIECES = 2
SLOTS = 3
TILE = 512
F32 = jnp.float32


def block_kernel(
    n, x_hbm, wg_hbm, wu_hbm, wd_hbm, y_hbm,
    xs, hidden, wtile, wd, arrived, leaving,
    x_sem, w_sem, wd_sem, y_sem, gs_sem, gr_sem, rs_sem, rr_sem, credit,
):
    rows, depth = x_hbm.shape
    units = wd_hbm.shape[0]
    tiles = units // LANES
    half = depth // 2
    chunks = half // TILE
    far = n // 2
    passes = far + 1
    me = lax.axis_index("tp")
    to = (lax.rem(me + 1, n), lax.rem(me + n - 1, n))
    source = (to[1], to[0])
    piece_rows = rows // PIECES

    def slot_of(d, hop):
        return n - 1 if hop == far else 2 * hop - 1 + d

    def piece_of(d, c):
        return c if d == 0 else PIECES - 1 - c

    def gather_copy(d, hop, c):
        at = pl.ds(piece_of(d, c) * piece_rows, piece_rows)
        src = x_hbm.at[at] if hop == 1 else xs.at[slot_of(d, hop - 1), at]
        return pltpu.make_async_remote_copy(
            src_ref=src,
            dst_ref=xs.at[slot_of(d, hop), at],
            send_sem=gs_sem.at[d, hop - 1, c],
            recv_sem=gr_sem.at[d, hop - 1, c],
            device_id={"tp": to[d]},
            device_id_type=pl.DeviceIdType.MESH,
        )

    def pieces_at(hop):
        return PIECES // 2 if hop == far else PIECES

    def receive_and_forward(hop):
        for c in range(pieces_at(hop)):
            for d in (0, 1):
                gather_copy(d, hop, c).wait_recv()
                if hop < far and c < pieces_at(hop + 1):
                    gather_copy(d, hop + 1, c).start()

    def weight_copies(t):
        slot = lax.rem(t, SLOTS)
        cols = pl.ds(pl.multiple_of(lax.rem(t, tiles) * LANES, LANES), LANES)
        return (
            pltpu.make_async_copy(wg_hbm.at[:, cols], wtile.at[slot, :, pl.ds(0, LANES)], w_sem.at[0, slot]),
            pltpu.make_async_copy(wu_hbm.at[:, cols], wtile.at[slot, :, pl.ds(LANES, LANES)], w_sem.at[1, slot]),
        )

    def start_weights(t):
        for copy in weight_copies(t):
            copy.start()

    def gate_up(number, slots, owners):
        def body(j, carry):
            t = number * tiles + j
            for copy in weight_copies(t):
                copy.wait()
            ahead = t + SLOTS - 1

            @pl.when(ahead < passes * tiles)
            def _():
                start_weights(ahead)

            if len(slots) == 1:
                block = xs[slots[0]]
            else:
                block = xs[slots[0] : slots[0] + 2].reshape(2 * rows, depth)
            both = jnp.dot(block, wtile[lax.rem(t, SLOTS)], preferred_element_type=F32)
            h = (jax.nn.silu(both[:, :LANES]) * both[:, LANES:]).astype(jnp.bfloat16)
            cols = pl.ds(pl.multiple_of(j * LANES, LANES), LANES)
            for i, owner in enumerate(owners):
                hidden[owner, :, cols] = h[i * rows : (i + 1) * rows]
            return carry

        lax.fori_loop(0, tiles, body, 0)

    def sum_copy(d, k, c):
        return pltpu.make_async_remote_copy(
            src_ref=leaving.at[d, c],
            dst_ref=arrived.at[d, lax.rem(k, 2), c],
            send_sem=rs_sem.at[d, c],
            recv_sem=rr_sem.at[d, lax.rem(k, 2), c],
            device_id={"tp": to[d]},
            device_id_type=pl.DeviceIdType.MESH,
        )

    def y_copy(d, c):
        cols = pl.ds(pl.multiple_of(d * half + c * TILE, TILE), TILE)
        return pltpu.make_async_copy(xs.at[0, :, cols], y_hbm.at[:, cols], y_sem.at[d, c])

    def sum_step(k, first=False, second=False, ends=False, gives=True):
        def body(c, carry):
            for d in (0, 1):
                owner = lax.rem(k + 1, n) if d == 0 else n - 1 - k
                cols = pl.ds(pl.multiple_of(d * half + c * TILE, TILE), TILE)
                acc = jnp.dot(hidden[owner], wd[:, cols], preferred_element_type=F32)
                if not first:
                    sum_copy(d, k - 1, c).wait_recv()
                    acc = acc + arrived[d, lax.rem(k - 1, 2), c].astype(F32)
                    sum_copy(d, k - 1, c).wait_send()
                if ends:
                    xs[0, :, cols] = acc.astype(jnp.bfloat16)
                else:
                    if not first and not second:
                        pl.semaphore_wait(credit.at[d, c], 1)
                    leaving[d, c] = acc.astype(jnp.bfloat16)
                    if not first and gives:
                        pl.semaphore_signal(
                            credit.at[d, c], inc=1, device_id={"tp": source[d]}, device_id_type=pl.DeviceIdType.MESH
                        )

            @pl.when(c > 0)
            def _():
                for d in (0, 1):
                    (y_copy(d, c - 1) if ends else sum_copy(d, k, c - 1)).start()

            return carry

        lax.fori_loop(0, chunks, body, 0)
        for d in (0, 1):
            (y_copy(d, chunks - 1) if ends else sum_copy(d, k, chunks - 1)).start()

    barrier = pltpu.get_barrier_semaphore()
    for device in to:
        pl.semaphore_signal(barrier, inc=1, device_id={"tp": device}, device_id_type=pl.DeviceIdType.MESH)
    own = pltpu.make_async_copy(x_hbm, xs.at[0], x_sem)
    own.start()
    for t in range(SLOTS - 1):
        start_weights(jnp.int32(t))
    pl.semaphore_wait(barrier, 2)
    for c in range(PIECES):
        for d in (0, 1):
            gather_copy(d, 1, c).start()
    own.wait()
    gate_up(0, (0,), (0,))
    down = pltpu.make_async_copy(wd_hbm, wd, wd_sem)
    down.start()
    for hop in range(1, far):
        receive_and_forward_now = hop < far - 1
        if receive_and_forward_now:
            receive_and_forward(hop)
        else:
            down.wait()
            sum_step(jnp.int32(0), first=True)
            receive_and_forward(hop)
        gate_up(hop, (slot_of(0, hop), slot_of(1, hop)), (hop, n - hop))
    sum_step(jnp.int32(1), second=True)
    receive_and_forward(far)
    gate_up(far, (n - 1,), (far,))

    def middle(k, carry):
        sum_step(k)
        return carry

    lax.fori_loop(2, n - 2, middle, 0)
    sum_step(jnp.int32(n - 2), gives=False)
    sum_step(jnp.int32(n - 1), ends=True)
    for d in (0, 1):
        for hop in range(1, far + 1):
            for c in range(pieces_at(hop)):
                gather_copy(d, hop, c).wait_send()
        for c in range(chunks):
            y_copy(d, c).wait()


def solution(mesh):
    n = mesh.shape["tp"]

    def step(x, w_gate, w_up, w_down):
        rows, depth = x.shape
        units = w_down.shape[0]
        chunks = depth // 2 // TILE
        bf16 = jnp.bfloat16
        dma = pltpu.SemaphoreType.DMA
        return pl.pallas_call(
            functools.partial(block_kernel, n),
            out_shape=jax.ShapeDtypeStruct((rows, depth), bf16),
            in_specs=[pl.BlockSpec(memory_space=pl.ANY)] * 4,
            out_specs=pl.BlockSpec(memory_space=pl.ANY),
            scratch_shapes=[
                pltpu.VMEM((n, rows, depth), bf16),
                pltpu.VMEM((n, rows, units), bf16),
                pltpu.VMEM((SLOTS, depth, 2 * LANES), bf16),
                pltpu.VMEM((units, depth), bf16),
                pltpu.VMEM((2, 2, chunks, rows, TILE), bf16),
                pltpu.VMEM((2, chunks, rows, TILE), bf16),
                dma,
                dma((2, SLOTS)),
                dma,
                dma((2, chunks)),
                dma((2, n // 2, PIECES)),
                dma((2, n // 2, PIECES)),
                dma((2, chunks)),
                dma((2, 2, chunks)),
                pltpu.SemaphoreType.REGULAR((2, chunks)),
            ],
            compiler_params=pltpu.CompilerParams(
                collective_id=0, has_side_effects=True, vmem_limit_bytes=67043328
            ),
            name="mlp_block",
        )(x, w_gate, w_up, w_down)

    return jax.shard_map(
        step,
        mesh=mesh,
        in_specs=(P(("dp", "tp"), None), P(None, "tp"), P(None, "tp"), P("tp", None)),
        out_specs=P(("dp", "tp"), None),
        check_vma=False,
    )
```

```python
import functools

import jax
import jax.numpy as jnp
from jax import lax
from jax.experimental import pallas as pl
from jax.experimental.pallas import tpu as pltpu
from jax.sharding import PartitionSpec as P

LANES = 128
PIECES = 2
SLOTS = 3
TILE = 512
F32 = jnp.float32


def block_kernel(
    n, x_hbm, wg_hbm, wu_hbm, wd_hbm, y_ref,
    xs, hidden, wtile, wd, arrived, leaving, term,
    x_sem, w_sem, wd_sem, gs_sem, gr_sem, rs_sem, rr_sem, credit,
):
    rows, depth = x_hbm.shape
    units = wd_hbm.shape[0]
    tiles = units // LANES
    half = depth // 2
    chunks = half // TILE
    far = n // 2
    passes = far + 1
    me = lax.axis_index("tp")
    to = (lax.rem(me + 1, n), lax.rem(me + n - 1, n))
    source = (to[1], to[0])
    piece_rows = rows // PIECES

    def slot_of(d, hop):
        return n - 2 if hop == far else 2 * hop - 2 + d

    def piece_of(d, c):
        return c if d == 0 else PIECES - 1 - c

    def gather_copy(d, hop, c):
        at = pl.ds(piece_of(d, c) * piece_rows, piece_rows)
        src = x_hbm.at[at] if hop == 1 else xs.at[slot_of(d, hop - 1), at]
        return pltpu.make_async_remote_copy(
            src_ref=src,
            dst_ref=xs.at[slot_of(d, hop), at],
            send_sem=gs_sem.at[d, hop - 1, c],
            recv_sem=gr_sem.at[d, hop - 1, c],
            device_id={"tp": to[d]},
            device_id_type=pl.DeviceIdType.MESH,
        )

    def pieces_at(hop):
        return PIECES // 2 if hop == far else PIECES

    def receive_and_forward(hop):
        for c in range(pieces_at(hop)):
            for d in (0, 1):
                gather_copy(d, hop, c).wait_recv()
                if hop < far and c < pieces_at(hop + 1):
                    gather_copy(d, hop + 1, c).start()

    def weight_copies(t):
        slot = lax.rem(t, SLOTS)
        cols = pl.ds(pl.multiple_of(lax.rem(t, tiles) * LANES, LANES), LANES)
        return (
            pltpu.make_async_copy(wg_hbm.at[:, cols], wtile.at[slot, :, pl.ds(0, LANES)], w_sem.at[0, slot]),
            pltpu.make_async_copy(wu_hbm.at[:, cols], wtile.at[slot, :, pl.ds(LANES, LANES)], w_sem.at[1, slot]),
        )

    def start_weights(t):
        for copy in weight_copies(t):
            copy.start()

    def gate_up(number, slots, owners):
        def body(j, carry):
            t = number * tiles + j
            for copy in weight_copies(t):
                copy.wait()
            ahead = t + SLOTS - 1

            @pl.when(ahead < passes * tiles)
            def _():
                start_weights(ahead)

            if not slots:
                block = y_ref[...]
            elif len(slots) == 1:
                block = xs[slots[0]]
            else:
                block = xs[slots[0] : slots[0] + 2].reshape(2 * rows, depth)
            both = jnp.dot(block, wtile[lax.rem(t, SLOTS)], preferred_element_type=F32)
            h = (jax.nn.silu(both[:, :LANES]) * both[:, LANES:]).astype(jnp.bfloat16)
            cols = pl.ds(pl.multiple_of(j * LANES, LANES), LANES)
            for i, owner in enumerate(owners):
                hidden[owner, :, cols] = h[i * rows : (i + 1) * rows]
            return carry

        lax.fori_loop(0, tiles, body, 0)

    def sum_copy(d, k, c):
        return pltpu.make_async_remote_copy(
            src_ref=leaving.at[d, c],
            dst_ref=arrived.at[d, lax.rem(k, 2), c],
            send_sem=rs_sem.at[d, c],
            recv_sem=rr_sem.at[d, lax.rem(k, 2), c],
            device_id={"tp": to[d]},
            device_id_type=pl.DeviceIdType.MESH,
        )

    def sum_step(k, first=False, second=False, ends=False):
        def body(c, carry):
            def cols(d):
                return pl.ds(pl.multiple_of(d * half + c * TILE, TILE), TILE)

            for d in (0, 1):
                owner = lax.rem(k + 1, n) if d == 0 else n - 1 - k
                term[d] = jnp.dot(hidden[owner], wd[:, cols(d)], preferred_element_type=F32)

            if not ends:

                @pl.when(c > 0)
                def _():
                    for d in (0, 1):
                        sum_copy(d, k, c - 1).start()

            for d in (0, 1):
                total = term[d]
                if not first:
                    sum_copy(d, k - 1, c).wait_recv()
                    total = total + arrived[d, lax.rem(k - 1, 2), c].astype(F32)
                    sum_copy(d, k - 1, c).wait_send()
                if ends:
                    y_ref[:, cols(d)] = total.astype(jnp.bfloat16)
                else:
                    if not first and not second:
                        pl.semaphore_wait(credit.at[d, c], 1)
                    leaving[d, c] = total.astype(jnp.bfloat16)
                    if not first:

                        @pl.when(k < n - 2)
                        def _():
                            pl.semaphore_signal(
                                credit.at[d, c], inc=1, device_id={"tp": source[d]}, device_id_type=pl.DeviceIdType.MESH
                            )

            return carry

        lax.fori_loop(0, chunks, body, 0)
        if not ends:
            for d in (0, 1):
                sum_copy(d, k, chunks - 1).start()

    barrier = pltpu.get_barrier_semaphore()
    for device in to:
        pl.semaphore_signal(barrier, inc=1, device_id={"tp": device}, device_id_type=pl.DeviceIdType.MESH)
    own = pltpu.make_async_copy(x_hbm, y_ref, x_sem)
    own.start()
    for t in range(SLOTS - 1):
        start_weights(jnp.int32(t))
    pl.semaphore_wait(barrier, 2)
    for c in range(PIECES):
        for d in (0, 1):
            gather_copy(d, 1, c).start()
    own.wait()
    gate_up(0, (), (0,))
    down = pltpu.make_async_copy(wd_hbm, wd, wd_sem)
    down.start()
    for hop in range(1, far):
        receive_and_forward_now = hop < far - 1
        if receive_and_forward_now:
            receive_and_forward(hop)
        else:
            down.wait()
            sum_step(jnp.int32(0), first=True)
            receive_and_forward(hop)
        gate_up(hop, (slot_of(0, hop), slot_of(1, hop)), (hop, n - hop))
    sum_step(jnp.int32(1), second=True)
    receive_and_forward(far)
    gate_up(far, (n - 2,), (far,))

    def middle(k, carry):
        sum_step(k)
        return carry

    lax.fori_loop(2, n - 1, middle, 0)
    sum_step(jnp.int32(n - 1), ends=True)
    for d in (0, 1):
        for hop in range(1, far + 1):
            for c in range(pieces_at(hop)):
                gather_copy(d, hop, c).wait_send()


def solution(mesh):
    n = mesh.shape["tp"]

    def step(x, w_gate, w_up, w_down):
        rows, depth = x.shape
        units = w_down.shape[0]
        chunks = depth // 2 // TILE
        bf16 = jnp.bfloat16
        dma = pltpu.SemaphoreType.DMA
        return pl.pallas_call(
            functools.partial(block_kernel, n),
            out_shape=pltpu.VMEM((rows, depth), bf16),
            in_specs=[pl.BlockSpec(memory_space=pl.ANY)] * 4,
            out_specs=pl.BlockSpec(memory_space=pltpu.VMEM),
            scratch_shapes=[
                pltpu.VMEM((n - 1, rows, depth), bf16),
                pltpu.VMEM((n, rows, units), bf16),
                pltpu.VMEM((SLOTS, depth, 2 * LANES), bf16),
                pltpu.VMEM((units, depth), bf16),
                pltpu.VMEM((2, 2, chunks, rows, TILE), bf16),
                pltpu.VMEM((2, chunks, rows, TILE), bf16),
                pltpu.VMEM((2, rows, TILE), F32),
                dma,
                dma((2, SLOTS)),
                dma,
                dma((2, n // 2, PIECES)),
                dma((2, n // 2, PIECES)),
                dma((2, chunks)),
                dma((2, 2, chunks)),
                pltpu.SemaphoreType.REGULAR((2, chunks)),
            ],
            compiler_params=pltpu.CompilerParams(
                collective_id=0, has_side_effects=True, vmem_limit_bytes=64500000
            ),
            name="mlp_block",
        )(x, w_gate, w_up, w_down)

    return jax.shard_map(
        step,
        mesh=mesh,
        in_specs=(P(("dp", "tp"), None), P(None, "tp"), P(None, "tp"), P("tp", None)),
        out_specs=P(("dp", "tp"), None),
        check_vma=False,
    )
```

```python
import functools

import jax
import jax.numpy as jnp
from jax import lax
from jax.experimental import pallas as pl
from jax.experimental.pallas import tpu as pltpu
from jax.sharding import PartitionSpec as P

LANES = 128
PIECES = 2
SLOTS = 3
TILE = 640
F32 = jnp.float32


def block_kernel(
    n, x_hbm, wg_hbm, wu_hbm, wd_hbm, y_ref,
    xs, hidden, wtile, wd, arrived, leaving, term,
    x_sem, w_sem, wd_sem, gs_sem, gr_sem, rs_sem, rr_sem, credit,
):
    rows, depth = x_hbm.shape
    units = wd_hbm.shape[0]
    tiles = units // LANES
    half = depth // 2
    chunks = half // TILE
    far = n // 2
    passes = far + 1
    me = lax.axis_index("tp")
    to = (lax.rem(me + 1, n), lax.rem(me + n - 1, n))
    source = (to[1], to[0])
    piece_rows = rows // PIECES

    def slot_of(d, hop):
        return n - 2 if hop == far else 2 * hop - 2 + d

    def piece_of(d, c):
        return c if d == 0 else PIECES - 1 - c

    def gather_copy(d, hop, c):
        at = pl.ds(piece_of(d, c) * piece_rows, piece_rows)
        src = x_hbm.at[at] if hop == 1 else xs.at[slot_of(d, hop - 1), at]
        return pltpu.make_async_remote_copy(
            src_ref=src,
            dst_ref=xs.at[slot_of(d, hop), at],
            send_sem=gs_sem.at[d, hop - 1, c],
            recv_sem=gr_sem.at[d, hop - 1, c],
            device_id={"tp": to[d]},
            device_id_type=pl.DeviceIdType.MESH,
        )

    def pieces_at(hop):
        return PIECES // 2 if hop == far else PIECES

    def receive_and_forward(hop):
        for c in range(pieces_at(hop)):
            for d in (0, 1):
                gather_copy(d, hop, c).wait_recv()
                if hop < far and c < pieces_at(hop + 1):
                    gather_copy(d, hop + 1, c).start()

    def weight_copies(t):
        slot = lax.rem(t, SLOTS)
        cols = pl.ds(pl.multiple_of(lax.rem(t, tiles) * LANES, LANES), LANES)
        return (
            pltpu.make_async_copy(wg_hbm.at[:, cols], wtile.at[slot, :, pl.ds(0, LANES)], w_sem.at[0, slot]),
            pltpu.make_async_copy(wu_hbm.at[:, cols], wtile.at[slot, :, pl.ds(LANES, LANES)], w_sem.at[1, slot]),
        )

    def start_weights(t):
        for copy in weight_copies(t):
            copy.start()

    def gate_up(number, slots, owners):
        def body(j, carry):
            t = number * tiles + j
            for copy in weight_copies(t):
                copy.wait()
            ahead = t + SLOTS - 1

            @pl.when(ahead < passes * tiles)
            def _():
                start_weights(ahead)

            if not slots:
                block = y_ref[...]
            elif len(slots) == 1:
                block = xs[slots[0]]
            else:
                block = xs[slots[0] : slots[0] + 2].reshape(2 * rows, depth)
            both = jnp.dot(block, wtile[lax.rem(t, SLOTS)], preferred_element_type=F32)
            h = (jax.nn.silu(both[:, :LANES]) * both[:, LANES:]).astype(jnp.bfloat16)
            cols = pl.ds(pl.multiple_of(j * LANES, LANES), LANES)
            for i, owner in enumerate(owners):
                hidden[owner, :, cols] = h[i * rows : (i + 1) * rows]
            return carry

        lax.fori_loop(0, tiles, body, 0)

    def sum_copy(d, k, c):
        return pltpu.make_async_remote_copy(
            src_ref=leaving.at[d, c],
            dst_ref=arrived.at[d, lax.rem(k, 2), c],
            send_sem=rs_sem.at[d, c],
            recv_sem=rr_sem.at[d, lax.rem(k, 2), c],
            device_id={"tp": to[d]},
            device_id_type=pl.DeviceIdType.MESH,
        )

    def sum_step(k, first=False, second=False, ends=False):
        def body(c, carry):
            def cols(d):
                return pl.ds(pl.multiple_of(d * half + c * TILE, TILE), TILE)

            for d in (0, 1):
                owner = lax.rem(k + 1, n) if d == 0 else n - 1 - k
                term[d] = jnp.dot(hidden[owner], wd[:, cols(d)], preferred_element_type=F32)

            if not ends:

                @pl.when(c > 0)
                def _():
                    for d in (0, 1):
                        sum_copy(d, k, c - 1).start()

            for d in (0, 1):
                total = term[d]
                if not first:
                    sum_copy(d, k - 1, c).wait_recv()
                    total = total + arrived[d, lax.rem(k - 1, 2), c].astype(F32)
                    if not ends:
                        sum_copy(d, k - 1, c).wait_send()
                if ends:
                    y_ref[:, cols(d)] = total.astype(jnp.bfloat16)
                else:
                    if not first and not second:
                        pl.semaphore_wait(credit.at[d, c], 1)
                    leaving[d, c] = total.astype(jnp.bfloat16)
                    if not first:

                        @pl.when(k < n - 2)
                        def _():
                            pl.semaphore_signal(
                                credit.at[d, c], inc=1, device_id={"tp": source[d]}, device_id_type=pl.DeviceIdType.MESH
                            )

            return carry

        lax.fori_loop(0, chunks, body, 0)
        for d in (0, 1):
            if ends:
                for c in range(chunks):
                    sum_copy(d, k - 1, c).wait_send()
            else:
                sum_copy(d, k, chunks - 1).start()

    barrier = pltpu.get_barrier_semaphore()
    for device in to:
        pl.semaphore_signal(barrier, inc=1, device_id={"tp": device}, device_id_type=pl.DeviceIdType.MESH)
    pl.semaphore_wait(barrier, 2)
    for c in range(PIECES):
        for d in (0, 1):
            gather_copy(d, 1, c).start()
    own = pltpu.make_async_copy(x_hbm, y_ref, x_sem)
    own.start()
    for t in range(SLOTS - 1):
        start_weights(jnp.int32(t))
    own.wait()
    gate_up(0, (), (0,))
    down = pltpu.make_async_copy(wd_hbm, wd, wd_sem)
    down.start()
    for hop in range(1, far):
        receive_and_forward_now = hop < far - 1
        if receive_and_forward_now:
            receive_and_forward(hop)
        else:
            down.wait()
            sum_step(jnp.int32(0), first=True)
            receive_and_forward(hop)
        gate_up(hop, (slot_of(0, hop), slot_of(1, hop)), (hop, n - hop))
    sum_step(jnp.int32(1), second=True)
    receive_and_forward(far)
    gate_up(far, (n - 2,), (far,))

    def middle(k, carry):
        sum_step(k)
        return carry

    lax.fori_loop(2, n - 1, middle, 0)
    sum_step(jnp.int32(n - 1), ends=True)
    for d in (0, 1):
        for hop in range(1, far + 1):
            for c in range(pieces_at(hop)):
                gather_copy(d, hop, c).wait_send()


def solution(mesh):
    n = mesh.shape["tp"]

    def step(x, w_gate, w_up, w_down):
        rows, depth = x.shape
        units = w_down.shape[0]
        chunks = depth // 2 // TILE
        bf16 = jnp.bfloat16
        dma = pltpu.SemaphoreType.DMA
        return pl.pallas_call(
            functools.partial(block_kernel, n),
            out_shape=pltpu.VMEM((rows, depth), bf16),
            in_specs=[pl.BlockSpec(memory_space=pl.ANY)] * 4,
            out_specs=pl.BlockSpec(memory_space=pltpu.VMEM),
            scratch_shapes=[
                pltpu.VMEM((n - 1, rows, depth), bf16),
                pltpu.VMEM((n, rows, units), bf16),
                pltpu.VMEM((SLOTS, depth, 2 * LANES), bf16),
                pltpu.VMEM((units, depth), bf16),
                pltpu.VMEM((2, 2, chunks, rows, TILE), bf16),
                pltpu.VMEM((2, chunks, rows, TILE), bf16),
                pltpu.VMEM((2, rows, TILE), F32),
                dma,
                dma((2, SLOTS)),
                dma,
                dma((2, n // 2, PIECES)),
                dma((2, n // 2, PIECES)),
                dma((2, chunks)),
                dma((2, 2, chunks)),
                pltpu.SemaphoreType.REGULAR((2, chunks)),
            ],
            compiler_params=pltpu.CompilerParams(
                collective_id=0, has_side_effects=True, vmem_limit_bytes=64500000
            ),
            name="mlp_block",
        )(x, w_gate, w_up, w_down)

    return jax.shard_map(
        step,
        mesh=mesh,
        in_specs=(P(("dp", "tp"), None), P(None, "tp"), P(None, "tp"), P("tp", None)),
        out_specs=P(("dp", "tp"), None),
        check_vma=False,
    )
```

```python
import functools

import jax
import jax.numpy as jnp
from jax import lax
from jax.experimental import pallas as pl
from jax.experimental.pallas import tpu as pltpu
from jax.sharding import PartitionSpec as P

LANES = 128
PIECES = 2
SLOTS = 3
TILE = 640
F32 = jnp.float32


def block_kernel(
    n, x_hbm, wg_hbm, wu_hbm, wd_hbm, y_ref,
    xs, hidden, wtile, wd, arrived, leaving, term,
    x_sem, w_sem, wd_sem, gs_sem, gr_sem, rs_sem, rr_sem, credit,
):
    rows, depth = x_hbm.shape
    units = wd_hbm.shape[0]
    tiles = units // LANES
    half = depth // 2
    chunks = half // TILE
    far = n // 2
    passes = far + 1
    me = lax.axis_index("tp")
    to = (lax.rem(me + 1, n), lax.rem(me + n - 1, n))
    source = (to[1], to[0])
    piece_rows = rows // PIECES

    def slot_of(d, hop):
        return n - 2 if hop == far else 2 * hop - 2 + d

    def piece_of(d, c):
        return c if d == 0 else PIECES - 1 - c

    def gather_copy(d, hop, c):
        at = pl.ds(piece_of(d, c) * piece_rows, piece_rows)
        src = x_hbm.at[at] if hop == 1 else xs.at[slot_of(d, hop - 1), at]
        return pltpu.make_async_remote_copy(
            src_ref=src,
            dst_ref=xs.at[slot_of(d, hop), at],
            send_sem=gs_sem.at[d, hop - 1, c],
            recv_sem=gr_sem.at[d, hop - 1, c],
            device_id={"tp": to[d]},
            device_id_type=pl.DeviceIdType.MESH,
        )

    def pieces_at(hop):
        return PIECES // 2 if hop == far else PIECES

    def receive_and_forward(hop):
        for c in range(pieces_at(hop)):
            for d in (0, 1):
                gather_copy(d, hop, c).wait_recv()
                if hop < far and c < pieces_at(hop + 1):
                    gather_copy(d, hop + 1, c).start()

    def weight_copies(t):
        slot = lax.rem(t, SLOTS)
        cols = pl.ds(pl.multiple_of(lax.rem(t, tiles) * LANES, LANES), LANES)
        return (
            pltpu.make_async_copy(wg_hbm.at[:, cols], wtile.at[slot, :, pl.ds(0, LANES)], w_sem.at[0, slot]),
            pltpu.make_async_copy(wu_hbm.at[:, cols], wtile.at[slot, :, pl.ds(LANES, LANES)], w_sem.at[1, slot]),
        )

    def start_weights(t):
        for copy in weight_copies(t):
            copy.start()

    def gate_up(number, slots, owners):
        def body(j, carry):
            t = number * tiles + j
            for copy in weight_copies(t):
                copy.wait()
            ahead = t + SLOTS - 1

            @pl.when(ahead < passes * tiles)
            def _():
                start_weights(ahead)

            if not slots:
                block = y_ref[...]
            elif len(slots) == 1:
                block = xs[slots[0]]
            else:
                block = xs[slots[0] : slots[0] + 2].reshape(2 * rows, depth)
            both = jnp.dot(block, wtile[lax.rem(t, SLOTS)], preferred_element_type=F32)
            h = (jax.nn.silu(both[:, :LANES]) * both[:, LANES:]).astype(jnp.bfloat16)
            cols = pl.ds(pl.multiple_of(j * LANES, LANES), LANES)
            for i, owner in enumerate(owners):
                hidden[owner, :, cols] = h[i * rows : (i + 1) * rows]
            return carry

        lax.fori_loop(0, tiles, body, 0)

    def sum_copy(d, k, c):
        return pltpu.make_async_remote_copy(
            src_ref=leaving.at[d, c],
            dst_ref=arrived.at[d, lax.rem(k, 2), c],
            send_sem=rs_sem.at[d, c],
            recv_sem=rr_sem.at[d, lax.rem(k, 2), c],
            device_id={"tp": to[d]},
            device_id_type=pl.DeviceIdType.MESH,
        )

    def sum_step(k, first=False, second=False, ends=False):
        def body(c, carry):
            def cols(d):
                return pl.ds(pl.multiple_of(d * half + c * TILE, TILE), TILE)

            for d in (0, 1):
                owner = lax.rem(k + 1, n) if d == 0 else n - 1 - k
                term[d] = jnp.dot(hidden[owner], wd[:, cols(d)], preferred_element_type=F32)

            @pl.when(c > 0)
            def _():
                for d in (0, 1):
                    if ends:
                        sum_copy(d, k - 1, c - 1).wait_send()
                    else:
                        sum_copy(d, k, c - 1).start()

            for d in (0, 1):
                total = term[d]
                if not first:
                    sum_copy(d, k - 1, c).wait_recv()
                    total = total + arrived[d, lax.rem(k - 1, 2), c].astype(F32)
                    if not ends:
                        sum_copy(d, k - 1, c).wait_send()
                if ends:
                    y_ref[:, cols(d)] = total.astype(jnp.bfloat16)
                else:
                    if not first and not second:
                        pl.semaphore_wait(credit.at[d, c], 1)
                    leaving[d, c] = total.astype(jnp.bfloat16)
                    if not first:

                        @pl.when(k < n - 2)
                        def _():
                            pl.semaphore_signal(
                                credit.at[d, c], inc=1, device_id={"tp": source[d]}, device_id_type=pl.DeviceIdType.MESH
                            )

            return carry

        lax.fori_loop(0, chunks, body, 0)
        for d in (0, 1):
            if ends:
                sum_copy(d, k - 1, chunks - 1).wait_send()
            else:
                sum_copy(d, k, chunks - 1).start()

    barrier = pltpu.get_barrier_semaphore()
    for device in to:
        pl.semaphore_signal(barrier, inc=1, device_id={"tp": device}, device_id_type=pl.DeviceIdType.MESH)
    pl.semaphore_wait(barrier, 2)
    for c in range(PIECES):
        for d in (0, 1):
            gather_copy(d, 1, c).start()
    own = pltpu.make_async_copy(x_hbm, y_ref, x_sem)
    own.start()
    for t in range(SLOTS - 1):
        start_weights(jnp.int32(t))
    own.wait()
    gate_up(0, (), (0,))
    down = pltpu.make_async_copy(wd_hbm, wd, wd_sem)
    down.start()
    for hop in range(1, far):
        receive_and_forward_now = hop < far - 1
        if receive_and_forward_now:
            receive_and_forward(hop)
        else:
            down.wait()
            sum_step(jnp.int32(0), first=True)
            receive_and_forward(hop)
        gate_up(hop, (slot_of(0, hop), slot_of(1, hop)), (hop, n - hop))
    sum_step(jnp.int32(1), second=True)
    receive_and_forward(far)
    gate_up(far, (n - 2,), (far,))

    def middle(k, carry):
        sum_step(k)
        return carry

    lax.fori_loop(2, n - 1, middle, 0)
    for d in (0, 1):
        for hop in range(1, far + 1):
            for c in range(pieces_at(hop)):
                gather_copy(d, hop, c).wait_send()
    sum_step(jnp.int32(n - 1), ends=True)


def solution(mesh):
    n = mesh.shape["tp"]

    def step(x, w_gate, w_up, w_down):
        rows, depth = x.shape
        units = w_down.shape[0]
        chunks = depth // 2 // TILE
        bf16 = jnp.bfloat16
        dma = pltpu.SemaphoreType.DMA
        return pl.pallas_call(
            functools.partial(block_kernel, n),
            out_shape=pltpu.VMEM((rows, depth), bf16),
            in_specs=[pl.BlockSpec(memory_space=pl.ANY)] * 4,
            out_specs=pl.BlockSpec(memory_space=pltpu.VMEM),
            scratch_shapes=[
                pltpu.VMEM((n - 1, rows, depth), bf16),
                pltpu.VMEM((n, rows, units), bf16),
                pltpu.VMEM((SLOTS, depth, 2 * LANES), bf16),
                pltpu.VMEM((units, depth), bf16),
                pltpu.VMEM((2, 2, chunks, rows, TILE), bf16),
                pltpu.VMEM((2, chunks, rows, TILE), bf16),
                pltpu.VMEM((2, rows, TILE), F32),
                dma,
                dma((2, SLOTS)),
                dma,
                dma((2, n // 2, PIECES)),
                dma((2, n // 2, PIECES)),
                dma((2, chunks)),
                dma((2, 2, chunks)),
                pltpu.SemaphoreType.REGULAR((2, chunks)),
            ],
            compiler_params=pltpu.CompilerParams(
                collective_id=0, has_side_effects=True, vmem_limit_bytes=64500000
            ),
            name="mlp_block",
        )(x, w_gate, w_up, w_down)

    return jax.shard_map(
        step,
        mesh=mesh,
        in_specs=(P(("dp", "tp"), None), P(None, "tp"), P(None, "tp"), P("tp", None)),
        out_specs=P(("dp", "tp"), None),
        check_vma=False,
    )
```
